8 devices in a mesh: rows: 8 (over z, y, x, core).
Axes of the slice: x: 2, y: 2, z: 1, core: 2. Of those that a mesh axis runs over, the one named last changes fastest.
Arguments:
- a_mat: float32 [16384, 256], P('rows')
- b_mat: float32 [16384, 4], P('rows')
Outputs:
- output 1: float32 [16384, 256], P('rows')
- output 2: float32 [256, 256], replicated
- output 3: float32 [256, 4], replicated
All inputs are finite; a program needn't handle non-finite values.
Results may differ from the reference program's by a relative error of at most 0.001.
Values sent between devices are 32-bit elements.
A program may use at most 1 GiB of HBM per device.

```python
import jax
import jax.numpy as jnp

NUM_BLOCKS = 8
ROWS_DEV = 2048
COLS = 256
RHS = 4

TOTAL_ROWS = NUM_BLOCKS * ROWS_DEV


def setup_inputs(seed: int = 0) -> dict:
    key = jax.random.key(seed)
    key_gauss, key_weight, key_left, key_right, key_rhs = jax.random.split(key, 5)
    gauss = jax.random.normal(key_gauss, (NUM_BLOCKS, ROWS_DEV, COLS), jnp.float32)
    col_weight = jnp.exp(jax.random.normal(key_weight, (NUM_BLOCKS, 1, COLS), jnp.float32))
    col_weight = col_weight / jnp.sqrt(jnp.mean(col_weight * col_weight, axis=2, keepdims=True))
    left_rot = jnp.linalg.qr(jax.random.normal(key_left, (COLS, COLS), jnp.float32))[0]
    right_rot = jnp.linalg.qr(jax.random.normal(key_right, (COLS, COLS), jnp.float32))[0]
    spread = 10.0 ** jnp.linspace(0.0, -2.5, COLS, dtype=jnp.float32)
    spread = spread / jnp.sqrt(jnp.mean(spread * spread))
    mixing = jnp.dot(left_rot * spread[None, :], right_rot.T)
    weighted = (gauss * col_weight).reshape(TOTAL_ROWS, COLS)
    a_mat = jnp.dot(weighted, mixing) * (TOTAL_ROWS ** -0.5)
    b_mat = jax.random.normal(key_rhs, (TOTAL_ROWS, RHS), jnp.float32)
    return {'a_mat': a_mat, 'b_mat': b_mat}


def reference(a_mat, b_mat):
    q_raw, r_raw = jnp.linalg.qr(a_mat)
    diag_signs = jnp.sign(jnp.diagonal(r_raw))
    q_fac = q_raw * diag_signs[None, :]
    r_fac = r_raw * diag_signs[:, None]
    c_mat = jnp.dot(q_fac.T, b_mat, preferred_element_type=jnp.float32)
    return q_fac, r_fac, c_mat
```

```python
import functools

import jax
import jax.numpy as jnp
from jax import lax
from jax.experimental import pallas as pl
from jax.experimental.pallas import tpu as pltpu
from jax.sharding import PartitionSpec as P

HI = lax.Precision.HIGHEST
F32 = jnp.float32
VM = pl.BlockSpec(memory_space=pltpu.VMEM)


def dot(x, y, dx, dy):
    return lax.dot_general(x, y, (((dx,), (dy,)), ((), ())), precision=HI, preferred_element_type=F32)


def bcast_row(x, i):
    return jnp.broadcast_to(x[i:i + 1, :], (8, x.shape[1]))

def factor(w_ref, n, nb, w):
    row8 = lax.broadcasted_iota(jnp.int32, (8, 128), 0)
    nt = nb // 8
    for k in range(n // nb):
        r0 = k * nb
        l0 = r0 // 128 * 128
        l1 = n + pl.cdiv(r0 + nb, 128) * 128
        wide = l1 - l0
        reps = wide // 128
        pan = [w_ref[r0 + 8 * t:r0 + 8 * t + 8, l0:l1] for t in range(nt)]
        scale = [None] * nt
        for b in range(nb // w):
            c0 = r0 + b * w - l0
            t0 = b * w // 8
            cols = [[jnp.broadcast_to(pan[t][:, c0 + j:c0 + j + 1], (8, 128)) if t >= t0 else None
                     for t in range(nt)] for j in range(w)]
            for j in range(w):
                jj = b * w + j
                tj, sj = jj // 8, jj % 8
                piv = bcast_row(cols[j][tj], sj)
                inv = lax.rsqrt(piv)
                lcol = [cols[j][t] * inv if t >= tj else None for t in range(nt)]
                lmul = list(lcol)
                lmul[tj] = jnp.where(row8 > sj, lcol[tj], 0.0)
                scale[tj] = inv if scale[tj] is None else jnp.where(row8 >= sj, inv, scale[tj])
                for j2 in range(j + 1, w):
                    q = b * w + j2
                    u = bcast_row(lcol[q // 8], q % 8)
                    for t in range(q // 8, nt):
                        cols[j2][t] = cols[j2][t] - lmul[t] * u
                urow = bcast_row(pan[tj], sj) * jnp.concatenate([inv] * reps, axis=1)
                for t in range(tj, nt):
                    pan[t] = pan[t] - jnp.concatenate([lmul[t]] * reps, axis=1) * urow
        done = jnp.concatenate([pan[t] * jnp.concatenate([scale[t]] * reps, axis=1) for t in range(nt)], axis=0)
        w_ref[r0:r0 + nb, l0:l1] = done
        r1 = r0 + nb
        if r1 < n:
            a0 = r1 // 128 * 128
            tall = done[:, a0 - l0:n - l0].T
            for lo, hi in ((r1, r1 + nb), (r1 + nb, n)):
                if lo < hi:
                    w_ref[lo:hi, l0:l1] -= jnp.dot(tall[lo - a0:hi - a0], done, precision=HI, preferred_element_type=F32)


def chol_kernel(nb, w, g_ref, u_ref, li_ref, w_ref):
    n = g_ref.shape[0]
    row = lax.broadcasted_iota(jnp.int32, (n, n), 0)
    col = lax.broadcasted_iota(jnp.int32, (n, n), 1)
    w_ref[:, :n] = g_ref[...]
    w_ref[:, n:] = jnp.where(row == col, 1.0, 0.0)
    factor(w_ref, n, nb, w)
    u_ref[...] = jnp.where(row <= col, w_ref[:, :n], 0.0)
    li_ref[...] = jnp.where(row >= col, w_ref[:, n:], 0.0)


def chol_inv(g):
    n = g.shape[0]
    return pl.pallas_call(
        functools.partial(chol_kernel, 32, 16),
        out_shape=[jax.ShapeDtypeStruct((n, n), F32)] * 2,
        in_specs=[VM], out_specs=[VM] * 2,
        scratch_shapes=[pltpu.VMEM((n, 2 * n), F32)],
        name="chol_inv",
    )(g)


def finish_kernel(q1_ref, g_ref, u_ref, c1_ref, q_ref, r_ref, c_ref, phi_ref, x_ref):
    n = g_ref.shape[0]
    row = lax.broadcasted_iota(jnp.int32, (n, n), 0)
    col = lax.broadcasted_iota(jnp.int32, (n, n), 1)
    half = jnp.where(row < col, 1.0, jnp.where(row == col, 0.5, 0.0))
    eye = jnp.where(row == col, 1.0, 0.0)
    dev = g_ref[...] - eye
    size = jnp.sqrt(jnp.sum(dev * dev))
    trips = jnp.where(size < 0.02, 3, 7)
    phi_ref[...] = dev * half

    def refine(_, carry):
        phi = phi_ref[...]
        phi_ref[...] = (dev - dot(phi, phi, 0, 0)) * half
        return carry

    lax.fori_loop(0, trips, refine, 0)
    phi = phi_ref[...]
    x_ref[...] = eye - phi

    def invert(_, carry):
        x_ref[...] = eye - dot(phi_ref[...], x_ref[...], 1, 0)
        return carry

    lax.fori_loop(0, trips, invert, 0)
    x = x_ref[...]
    r_ref[...] = jnp.where(row <= col, u_ref[...] + dot(phi, u_ref[...], 1, 0), 0.0)
    c_ref[...] = dot(x, c1_ref[...], 0, 0)
    q_ref[...] = dot(q1_ref[...], x, 1, 0)


def finish(q1, g, u, c1):
    n = g.shape[0]
    return pl.pallas_call(
        finish_kernel,
        out_shape=[jax.ShapeDtypeStruct(q1.shape, F32), jax.ShapeDtypeStruct((n, n), F32), jax.ShapeDtypeStruct(c1.shape, F32)],
        in_specs=[VM] * 4, out_specs=[VM] * 3,
        scratch_shapes=[pltpu.VMEM((n, n), F32)] * 2,
        name="finish",
    )(q1, g, u, c1)


def solution(mesh):
    def gram(q_blk, b_blk):
        g = dot(q_blk, q_blk, 0, 0)
        c = dot(q_blk, b_blk, 0, 0)
        return lax.psum(g, "rows"), lax.psum(c, "rows")

    def local_fn(a_blk, b_blk):
        n = a_blk.shape[1]
        eye = jnp.eye(n, dtype=F32)
        g0, _ = gram(a_blk, b_blk)
        u1, li = chol_inv(g0)
        q1 = dot(a_blk, li, 1, 1)
        g1, c1 = gram(q1, b_blk)

        def far(state):
            it, _, _, g, _, _, _ = state
            dev = g - eye
            return jnp.logical_and(jnp.logical_not(jnp.sum(dev * dev) < 0.01), it < 8)

        def again(state):
            it, q, u, g, c, a, b = state
            first = it == 0
            q = jnp.where(first, a, q)
            u = jnp.where(first, eye, u)
            g, _ = gram(q, b)
            step, inv = chol_inv(g + (2e-6 * jnp.trace(g)) * eye)
            q = dot(q, inv, 1, 1)
            u = dot(step, u, 1, 0)
            g, c = gram(q, b)
            return it + 1, q, u, g, c, a, b

        _, q1, u1, g1, c1, _, _ = lax.while_loop(far, again, (jnp.int32(0), q1, u1, g1, c1, a_blk, b_blk))
        return tuple(finish(q1, g1, u1, c1))

    return jax.shard_map(local_fn, mesh=mesh, in_specs=(P("rows", None), P("rows", None)), out_specs=(P("rows", None), P(), P()), check_vma=False)
```

```python
import functools

import jax
import jax.numpy as jnp
from jax import lax
from jax.experimental import pallas as pl
from jax.experimental.pallas import tpu as pltpu
from jax.sharding import PartitionSpec as P

HI = lax.Precision.HIGHEST
F32 = jnp.float32
VM = pl.BlockSpec(memory_space=pltpu.VMEM)
ANY = pl.BlockSpec(memory_space=pl.ANY)
SM = pl.BlockSpec(memory_space=pltpu.SMEM)
MESH = pl.DeviceIdType.MESH
CHUNK = 512
PACK = 416
HALF, QUARTER = PACK // 2, PACK // 4


def dot(x, y, dx, dy):
    return lax.dot_general(x, y, (((dx,), (dy,)), ((), ())), precision=HI, preferred_element_type=F32)


def bcast_row(x, i):
    return jnp.broadcast_to(x[i:i + 1, :], (8, x.shape[1]))

def factor(w_ref, n, nb, w):
    row8 = lax.broadcasted_iota(jnp.int32, (8, 128), 0)
    nt = nb // 8
    for k in range(n // nb):
        r0 = k * nb
        l0 = r0 // 128 * 128
        l1 = n + pl.cdiv(r0 + nb, 128) * 128
        wide = l1 - l0
        reps = wide // 128
        pan = [w_ref[r0 + 8 * t:r0 + 8 * t + 8, l0:l1] for t in range(nt)]
        scale = [None] * nt
        for b in range(nb // w):
            c0 = r0 + b * w - l0
            t0 = b * w // 8
            cols = [[jnp.broadcast_to(pan[t][:, c0 + j:c0 + j + 1], (8, 128)) if t >= t0 else None
                     for t in range(nt)] for j in range(w)]
            for j in range(w):
                jj = b * w + j
                tj, sj = jj // 8, jj % 8
                piv = bcast_row(cols[j][tj], sj)
                inv = lax.rsqrt(piv)
                lcol = [cols[j][t] * inv if t >= tj else None for t in range(nt)]
                lmul = list(lcol)
                lmul[tj] = jnp.where(row8 > sj, lcol[tj], 0.0)
                scale[tj] = inv if scale[tj] is None else jnp.where(row8 >= sj, inv, scale[tj])
                for j2 in range(j + 1, w):
                    q = b * w + j2
                    u = bcast_row(lcol[q // 8], q % 8)
                    for t in range(q // 8, nt):
                        cols[j2][t] = cols[j2][t] - lmul[t] * u
                urow = bcast_row(pan[tj], sj) * jnp.concatenate([inv] * reps, axis=1)
                for t in range(tj, nt):
                    pan[t] = pan[t] - jnp.concatenate([lmul[t]] * reps, axis=1) * urow
        done = jnp.concatenate([pan[t] * jnp.concatenate([scale[t]] * reps, axis=1) for t in range(nt)], axis=0)
        w_ref[r0:r0 + nb, l0:l1] = done
        r1 = r0 + nb
        if r1 < n:
            a0 = r1 // 128 * 128
            tall = done[:, a0 - l0:n - l0].T
            for lo, hi in ((r1, r1 + nb), (r1 + nb, n)):
                if lo < hi:
                    w_ref[lo:hi, l0:l1] -= jnp.dot(tall[lo - a0:hi - a0], done, precision=HI, preferred_element_type=F32)


def neighbours():
    me = lax.axis_index("rows")
    core, x, y = me % 2, me // 2 % 2, me // 4
    return core, (me + 1 - 2 * core, me + 2 - 4 * x, me + 4 - 8 * y)


def entry_barrier():
    barrier = pltpu.get_barrier_semaphore()
    for device in neighbours()[1]:
        pl.semaphore_signal(barrier, inc=1, device_id=(device,), device_id_type=MESH)
    pl.semaphore_wait(barrier, 3)


def all_reduce(part, total, bufs, send, recv):
    got0, mine1, got1, mine2, got2 = bufs
    core, (mate, x_dev, y_dev) = neighbours()
    keep = pl.multiple_of(core * HALF, 8)
    give = pl.multiple_of((1 - core) * HALF, 8)

    def copy(src, dst, k, device):
        return pltpu.make_async_remote_copy(
            src_ref=src, dst_ref=dst, send_sem=send.at[k], recv_sem=recv.at[k], device_id=(device,), device_id_type=MESH
        )

    c0 = copy(part.at[pl.ds(give, HALF)], got0, 0, mate)
    c0.start()
    c0.wait()
    for q in range(2):
        mine1[q] = part[pl.ds(pl.multiple_of(keep + q * QUARTER, 8), QUARTER)] + got0[q * QUARTER:(q + 1) * QUARTER]
    step1 = [copy(mine1.at[q], got1.at[q], 1 + q, (x_dev, y_dev)[q]) for q in range(2)]
    for c in step1:
        c.start()
    step2 = [copy(mine2.at[q], got2.at[q], 3 + q, (y_dev, x_dev)[q]) for q in range(2)]
    for q in range(2):
        step1[q].wait()
        mine2[q] = mine1[q] + got1[q]
        step2[q].start()
    for q in range(2):
        step2[q].wait()
        total[pl.ds(pl.multiple_of(keep + q * QUARTER, 8), QUARTER)] = mine2[q] + got2[q]
    c3 = copy(total.at[pl.ds(keep, HALF)], total.at[pl.ds(keep, HALF)], 5, mate)
    c3.start()
    c3.wait()


def pack_gram(part, g):
    part[0:128] = g[:128, :128]
    part[128:256] = g[:128, 128:]
    part[256:384] = g[128:, 128:]


def unpack_gram(total):
    top = jnp.concatenate([total[0:128], total[128:256]], axis=1)
    low = jnp.concatenate([total[128:256].T, total[256:384]], axis=1)
    return jnp.concatenate([top, low], axis=0)


def front_kernel(a_ref, bt_ref, shift_ref, q_ref, u_ref, g_ref, ct_ref, size_ref,
                 a_buf, q_buf, w_ref, x_ref, part, total, got0, mine1, got1, mine2, got2, a_sem, q_sem, send, recv):
    n = a_ref.shape[1]
    steps = a_ref.shape[0] // CHUNK
    row = lax.broadcasted_iota(jnp.int32, (n, n), 0)
    col = lax.broadcasted_iota(jnp.int32, (n, n), 1)
    loads = [pltpu.make_async_copy(a_ref.at[pl.ds(i * CHUNK, CHUNK)], a_buf.at[pl.ds(i * CHUNK, CHUNK)], a_sem.at[i])
             for i in range(steps)]
    for load in loads:
        load.start()
    entry_barrier()
    g = None
    for i in range(steps):
        loads[i].wait()
        blk = a_buf[i * CHUNK:(i + 1) * CHUNK]
        add = dot(blk, blk, 0, 0)
        g = add if g is None else g + add
    part[0, 384:] = jnp.zeros((PACK - 384, 128), F32)
    pack_gram(part.at[0], g)
    sets = [tuple(r.at[k] for r in (got0, mine1, got1, mine2, got2)) for k in range(2)]
    all_reduce(part.at[0], total.at[0], sets[0], send.at[0], recv.at[0])
    g = unpack_gram(total.at[0])
    w_ref[:, :n] = jnp.where(row == col, g * (1.0 + shift_ref[0, 0]), g)
    w_ref[:, n:] = jnp.where(row == col, 1.0, 0.0)
    factor(w_ref, n, 32, 16)
    u_ref[...] = jnp.where(row <= col, w_ref[:, :n], 0.0)
    x_ref[...] = jnp.where(row >= col, w_ref[:, n:], 0.0).T
    x = x_ref[...]
    g = ct = None
    stores = []
    for i in range(steps):
        rows = pl.ds(i * CHUNK, CHUNK)
        blk = dot(a_buf[rows], x, 1, 0)
        q_buf[rows] = blk
        store = pltpu.make_async_copy(q_buf.at[rows], q_ref.at[rows], q_sem.at[i])
        store.start()
        stores.append(store)
        add = dot(blk, blk, 0, 0)
        g = add if g is None else g + add
        add = dot(bt_ref[:, rows], blk, 1, 0)
        ct = add if ct is None else ct + add
    part[1, 384:] = jnp.zeros((PACK - 384, 128), F32)
    part[1, 384:388] = ct[:, :128]
    part[1, 392:396] = ct[:, 128:]
    pack_gram(part.at[1], g)
    all_reduce(part.at[1], total.at[1], sets[1], send.at[1], recv.at[1])
    g = unpack_gram(total.at[1])
    g_ref[...] = g
    ct_ref[...] = jnp.concatenate([total[1, 384:388], total[1, 392:396]], axis=1)
    dev = jnp.where(row == col, g - 1.0, g)
    size_ref[0, 0] = jnp.sum(dev * dev)
    for store in stores:
        store.wait()


def front(a, bt, shift):
    m, n = a.shape
    k = bt.shape[0]
    steps = m // CHUNK
    quarters = pltpu.VMEM((2, 2, QUARTER, 128), F32)
    return pl.pallas_call(
        front_kernel,
        out_shape=[jax.ShapeDtypeStruct((m, n), F32), jax.ShapeDtypeStruct((n, n), F32), jax.ShapeDtypeStruct((n, n), F32),
                   jax.ShapeDtypeStruct((k, n), F32), jax.ShapeDtypeStruct((1, 1), F32)],
        in_specs=[ANY, VM, SM], out_specs=[ANY, VM, VM, VM, SM],
        scratch_shapes=[
            pltpu.VMEM((m, n), F32), pltpu.VMEM((m, n), F32), pltpu.VMEM((n, 2 * n), F32), pltpu.VMEM((n, n), F32),
            pltpu.VMEM((2, PACK, 128), F32), pltpu.VMEM((2, PACK, 128), F32), pltpu.VMEM((2, HALF, 128), F32),
            quarters, quarters, quarters, quarters,
            pltpu.SemaphoreType.DMA((steps,)), pltpu.SemaphoreType.DMA((steps,)),
            pltpu.SemaphoreType.DMA((2, 6)), pltpu.SemaphoreType.DMA((2, 6)),
        ],
        compiler_params=pltpu.CompilerParams(collective_id=0, has_side_effects=True),
        name="front",
    )(a, bt, shift)


def finish_kernel(q1_ref, g_ref, u_ref, ct_ref, size_ref, q_ref, r_ref, c_ref, phi_ref, x_ref, in_buf, out_buf, in_sem, out_sem):
    n = g_ref.shape[0]
    steps = q1_ref.shape[0] // CHUNK
    parts = [pl.ds(i * CHUNK, CHUNK) for i in range(steps)]
    loads = [pltpu.make_async_copy(q1_ref.at[parts[i]], in_buf.at[parts[i]], in_sem.at[i]) for i in range(steps)]
    for load in loads:
        load.start()
    row = lax.broadcasted_iota(jnp.int32, (n, n), 0)
    col = lax.broadcasted_iota(jnp.int32, (n, n), 1)
    half = jnp.where(row < col, 1.0, jnp.where(row == col, 0.5, 0.0))
    eye = jnp.where(row == col, 1.0, 0.0)
    dev = g_ref[...] - eye
    trips = jnp.where(size_ref[0, 0] < 4e-4, 3, 7)
    phi_ref[...] = dev * half

    def refine(_, carry):
        phi = phi_ref[...]
        phi_ref[...] = (dev - dot(phi, phi, 0, 0)) * half
        return carry

    lax.fori_loop(0, trips, refine, 0)
    phi = phi_ref[...]
    x_ref[...] = eye - phi

    def invert(_, carry):
        x_ref[...] = eye - dot(phi_ref[...], x_ref[...], 1, 0)
        return carry

    lax.fori_loop(0, trips, invert, 0)
    x = x_ref[...]
    stores = []
    for i in range(steps):
        loads[i].wait()
        out_buf[parts[i]] = dot(in_buf[parts[i]], x, 1, 0)
        store = pltpu.make_async_copy(out_buf.at[parts[i]], q_ref.at[parts[i]], out_sem.at[i])
        store.start()
        stores.append(store)
    r_ref[...] = jnp.where(row <= col, u_ref[...] + dot(phi, u_ref[...], 1, 0), 0.0)
    c_ref[...] = dot(ct_ref[...], x, 1, 0)
    for store in stores:
        store.wait()


def finish(q1, g, u, ct, size):
    m, n = q1.shape
    steps = m // CHUNK
    return pl.pallas_call(
        finish_kernel,
        out_shape=[jax.ShapeDtypeStruct((m, n), F32), jax.ShapeDtypeStruct((n, n), F32), jax.ShapeDtypeStruct(ct.shape, F32)],
        in_specs=[ANY, VM, VM, VM, SM], out_specs=[ANY, VM, VM],
        scratch_shapes=[pltpu.VMEM((n, n), F32)] * 2 + [pltpu.VMEM((m, n), F32)] * 2 + [pltpu.SemaphoreType.DMA((steps,))] * 2,
        name="finish",
    )(q1, g, u, ct, size)


def solution(mesh):
    def local_fn(a_blk, b_blk):
        n = a_blk.shape[1]
        bt = b_blk.T
        q, u, g, ct, size = front(a_blk, bt, jnp.zeros((1, 1), F32))

        def far(state):
            it, _, _, _, _, size, _, _ = state
            return jnp.logical_and(jnp.logical_not(size[0, 0] < 0.01), it < 8)

        def again(state):
            it, q, u, _, _, _, a, bt = state
            first = it == 0
            q = jnp.where(first, a, q)
            u = jnp.where(first, jnp.eye(n, dtype=F32), u)
            q, step, g, ct, size = front(q, bt, jnp.full((1, 1), 1e-5, F32))
            return it + 1, q, dot(step, u, 1, 0), g, ct, size, a, bt

        _, q, u, g, ct, size, _, _ = lax.while_loop(far, again, (jnp.int32(0), q, u, g, ct, size, a_blk, bt))
        q, r, c = finish(q, g, u, ct, size)
        return q, r, c.T

    return jax.shard_map(local_fn, mesh=mesh, in_specs=(P("rows", None), P("rows", None)), out_specs=(P("rows", None), P(), P()), check_vma=False)
```
